32 devices in a mesh: region: 2 (over x), dev: 16 (over z, y, core).
Axes of the slice: x: 2, y: 2, z: 4, core: 2. Of those that a mesh axis runs over, the one named last changes fastest.
Arguments:
- object_field: float32 [2, 8192, 512], P(None, ('region', 'dev')), may hold values from -6 to 6
- probe: float32 [2, 256, 256], replicated, may hold values from -6 to 6
- amplitudes: float32 [2, 16, 4, 256, 256], P('region', 'dev'), may hold values from 0.5 to 4
- row_offset: int32 [2, 16, 4], P('region', 'dev'), may hold values from 0 to 255
- col_offset: int32 [2, 16, 4], P('region', 'dev'), may hold values from 0 to 256
- frame_count: int32 [2, 16], P('region', 'dev'), may hold values from 1 to 4, as said below
Outputs:
- new_object: float32 [2, 8192, 512], P(None, ('region', 'dev'))
- new_probe: float32 [2, 256, 256], replicated
The draws below stay inside these ranges and needn't reach their ends.
Inputs may be any that keep to these rules, and one draw needn't show every extreme that they name: `frame_count`: in each region, device j and device j + 8 together hold at most 6 frames, and some device holds 4.
All inputs are finite; a program needn't handle non-finite values.
Results may differ from the reference program's by a relative error of at most 0.0003.
Values sent between devices are 32-bit elements; how exact they have to be, the bound alone decides.
A program may use at most 64 MiB of HBM per device.

```python
import jax
import jax.numpy as jnp
from jax import lax

FRAME = 256
BAND = 256
WIDTH = 512
FRAMES_DEV = 4
ITERS = 1
REGIONS = 2
DEVS = 16
ROWS = 8192
N_REGION = 2
N_DEV = 16


def draw_frame_count(key, part):
    half_devs = DEVS // 2
    streams = jax.random.split(jax.random.fold_in(key, 11), 4)
    heavy = jax.random.randint(streams[0], (REGIONS, half_devs), FRAMES_DEV // 2, FRAMES_DEV + 1)
    forced = jax.random.randint(streams[1], (REGIONS, 1), 0, half_devs)
    heavy = jnp.where(jnp.arange(half_devs)[None, :] == forced, FRAMES_DEV, heavy)
    ceiling = jnp.minimum(FRAMES_DEV, FRAMES_DEV + FRAMES_DEV // 2 - heavy)
    light = jax.random.randint(streams[2], (REGIONS, half_devs), 1, ceiling + 1)
    flips = jax.random.randint(streams[3], (REGIONS, half_devs), 0, 2)
    first_half = jnp.where(flips == 1, heavy, light)
    second_half = jnp.where(flips == 1, light, heavy)
    return jnp.concatenate([first_half, second_half], axis=1).astype(jnp.int32)


def place_ends(drawn, stream_key, smallest, high):
    shape = drawn.shape
    place = [jax.random.randint(jax.random.fold_in(stream_key, axis), (), 0, shape[axis]) for axis in range(len(shape))]
    drawn = drawn.at[tuple(place)].set(smallest)
    longest = shape.index(max(shape))
    place[longest] = (place[longest] + 1) % shape[longest]
    return drawn.at[tuple(place)].set(high)


def shard_levels(own_key, dims, cuts, least, high):
    gain, own = 1.0, jax.random.fold_in(own_key, 6)
    for axis_at, parts in cuts:
        steps = jnp.exp(jax.random.uniform(jax.random.fold_in(own, axis_at), (parts,), jnp.float32, least / len(cuts), high / len(cuts)))
        gain = gain * jnp.repeat(steps, dims[axis_at] // parts).reshape([-1 if axis == axis_at else 1 for axis in range(len(dims))])
    return gain


def bell_draw(key, shape, width, bound, shards=(), held_as=jnp.bfloat16):
    array = width * jax.random.normal(key, shape, jnp.float32)
    if shards:
        array = array * shard_levels(key, shape, shards, -0.22, 0.18)
    return jnp.clip(array, -bound, bound).astype(held_as)


def setup_inputs(seed: int = 0) -> dict:
    keys = jax.random.split(jax.random.key(seed), 7)
    object_field = bell_draw(keys[0], (2, ROWS, WIDTH), 1.0, 6.0, ((1, 32),), jnp.float32)
    probe = bell_draw(keys[1], (2, FRAME, FRAME), 1.0, 6.0, (), jnp.float32)
    amplitudes = jnp.clip(0.5 + 3.5 * jax.random.uniform(keys[2], (REGIONS, DEVS, FRAMES_DEV, FRAME, FRAME), jnp.float32) ** shard_levels(keys[2], (REGIONS, DEVS, FRAMES_DEV, FRAME, FRAME), ((0, 2), (1, 16)), -0.2, 0.2), 0.5, 4.0)
    row_offset = place_ends(jax.random.randint(keys[3], (REGIONS, DEVS, FRAMES_DEV), 0, BAND), jax.random.fold_in(keys[3], 1), 0, BAND - 1).astype(jnp.int32)
    col_offset = place_ends(jax.random.randint(keys[4], (REGIONS, DEVS, FRAMES_DEV), 0, WIDTH - FRAME + 1), jax.random.fold_in(keys[4], 1), 0, WIDTH - FRAME).astype(jnp.int32)
    frame_count = draw_frame_count(jax.random.fold_in(keys[6], 71), 0)
    return {"object_field": object_field, "probe": probe, "amplitudes": amplitudes, "row_offset": row_offset, "col_offset": col_offset, "frame_count": frame_count}


def fourier_wave(windows, probe, measured, live_mask):
    object_wave = windows[:, 0] + 1j * windows[:, 1]
    probe_wave = probe[0] + 1j * probe[1]
    spectrum = jnp.fft.fft2(probe_wave[None] * object_wave, norm='ortho')
    modulus = jnp.sqrt(jnp.real(spectrum) ** 2 + jnp.imag(spectrum) ** 2 + 0.25)
    corrected = spectrum * (1.0 - measured / modulus)
    returned = jnp.fft.ifft2(corrected, norm='ortho') * live_mask[:, None, None]
    return (jnp.real(returned), jnp.imag(returned))

def region_pass(region_object, probe, measured, row_starts, col_starts, live_mask):
    span_rows = region_object.shape[1]
    padded = jnp.pad(region_object, ((0, 0), (0, FRAME), (0, 0)))

    def window_cut(row_start, col_start):
        return lax.dynamic_slice(padded, (jnp.int32(0), row_start.astype(jnp.int32), col_start.astype(jnp.int32)), (2, FRAME, FRAME))
    windows = jax.vmap(window_cut)(row_starts, col_starts)
    back_real, back_imag = fourier_wave(windows, probe, measured, live_mask)
    grad_real = lax.optimization_barrier(jnp.sum(windows[:, 0] * back_real + windows[:, 1] * back_imag, axis=0))
    grad_imag = lax.optimization_barrier(jnp.sum(windows[:, 0] * back_imag - windows[:, 1] * back_real, axis=0))
    power = probe[0] * probe[0] + probe[1] * probe[1]
    pieces = jnp.stack([probe[0] * back_real + probe[1] * back_imag, probe[0] * back_imag - probe[1] * back_real, power[None] * live_mask[:, None, None]], axis=1)

    def accumulate(index, totals):
        row_start = row_starts[index].astype(jnp.int32)
        col_start = col_starts[index].astype(jnp.int32)
        anchor = (jnp.int32(0), row_start, col_start)
        current = lax.dynamic_slice(totals, anchor, (3, FRAME, FRAME))
        return lax.dynamic_update_slice(totals, current + pieces[index], anchor)
    totals = lax.fori_loop(0, pieces.shape[0], accumulate, jnp.zeros((3, span_rows + FRAME, region_object.shape[2]), jnp.float32))
    updated = region_object - totals[:2, :span_rows] / (totals[2:3, :span_rows] + 1.0)
    return (updated, jnp.stack([grad_real, grad_imag]))

def reference(object_field, probe, amplitudes, row_offset, col_offset, frame_count):
    span_rows = N_DEV * BAND
    regions = object_field.reshape(2, N_REGION, span_rows, WIDTH).transpose(1, 0, 2, 3)
    band_starts = (jnp.arange(N_DEV, dtype=jnp.int32) * BAND)[None, :, None]
    row_starts = (row_offset + band_starts).astype(jnp.int32).reshape(N_REGION, -1)
    col_starts = col_offset.astype(jnp.int32).reshape(N_REGION, -1)
    slot_index = jnp.arange(FRAMES_DEV, dtype=jnp.int32)[None, None, :]
    live_mask = (slot_index < frame_count[:, :, None]).astype(jnp.float32).reshape(N_REGION, -1)
    measured = amplitudes.reshape(N_REGION, -1, FRAME, FRAME)
    for iteration in range(ITERS):
        current_probe = probe

        def one_region(inputs):
            return region_pass(inputs[0], current_probe, inputs[1], inputs[2], inputs[3], inputs[4])
        regions, gradients = lax.map(one_region, (regions, measured, row_starts, col_starts, live_mask))
        summed = lax.optimization_barrier(jnp.sum(gradients, axis=0))
        spread = jnp.sqrt(jnp.mean(summed * summed) + 1e-06)
        probe = probe - 0.25 * summed / spread
    new_object = regions.transpose(1, 0, 2, 3).reshape(2, N_REGION * span_rows, WIDTH)
    return (new_object, probe)
```

```python
import math

import jax
import jax.numpy as jnp
import numpy as np
from jax import lax
from jax.experimental import pallas as pl
from jax.experimental.pallas import tpu as pltpu
from jax.sharding import PartitionSpec as P

PAD = 8


def from_behind(array, axis, by):
    peers = lax.axis_size(axis)
    pairs = [(i, i + by) for i in range(peers) if 0 <= i + by < peers]
    return lax.ppermute(array, axis, pairs)


def split(x):
    high = x.astype(jnp.bfloat16)
    return high, (x - high.astype(jnp.float32)).astype(jnp.bfloat16)


def fourier_tables(length):
    index = np.arange(length)
    angle = (index[:, None] * index[None, :] % length) * (2.0 * math.pi / length)
    factor = 1.0 / math.sqrt(length)
    cosine = np.cos(angle) * factor
    sine = np.sin(angle) * factor
    parts = []
    for table in (cosine, sine, cosine + sine, cosine - sine):
        table = table.astype(np.float32)
        high = table.astype(jnp.bfloat16)
        parts += [high, (table - high.astype(np.float32)).astype(jnp.bfloat16)]
    return jnp.asarray(np.stack(parts))


def dot(a, b):
    return jnp.dot(a, b, preferred_element_type=jnp.float32)


def product(tables, which, x, left):
    t_high, t_low = tables[2 * which], tables[2 * which + 1]
    high, low = split(x)
    if left:
        return dot(t_high, high) + (dot(t_high, low) + dot(t_low, high))
    return dot(high, t_high) + (dot(low, t_high) + dot(high, t_low))


def side(tables, real, imag, inverse, left):
    first = product(tables, 2 if inverse else 3, real, left)
    second = product(tables, 0, imag - real, left)
    third = product(tables, 1, real + imag, left)
    if inverse:
        return first - third, first + second
    return first + third, first + second


def kernel(
    rows_s, cols_s, count_s, prior_s, field, rim, probe, measured, tables,
    totals, weight, grad, extended, spread,
):
    band, width = field.shape[1], field.shape[2]
    frame = probe.shape[1]
    slots = rows_s.shape[0]
    tall = frame + PAD
    extended[:, :band] = field[...]
    extended[:, band:] = rim[...]
    totals[...] = jnp.zeros_like(totals)
    spread[...] = jnp.zeros_like(spread)
    grad[...] = jnp.zeros_like(grad)

    def anchor(row):
        base = pl.multiple_of(row // PAD * PAD, PAD)
        return pl.ds(base, tall), row - base

    def cut(plane, row, col):
        at, shift = anchor(row)
        x = extended[plane, at, :]
        x = pltpu.roll(x, lax.rem(width - col, width), 1)[:, :frame]
        return pltpu.roll(x, lax.rem(tall - shift, tall), 0)[:frame]

    def place(x, row, col):
        at, shift = anchor(row)
        x = jnp.concatenate([x, jnp.zeros((PAD, frame), jnp.float32)], axis=0)
        x = pltpu.roll(x, shift, 0)
        x = jnp.concatenate([x, jnp.zeros((tall, width - frame), jnp.float32)], axis=1)
        return at, pltpu.roll(x, col, 1)

    def power():
        return probe[0] * probe[0] + probe[1] * probe[1]

    def prior(k, carry):
        at, x = place(power(), prior_s[k], prior_s[slots + k])
        spread[at, :] += x
        return carry

    lax.fori_loop(0, prior_s[2 * slots], prior, 0)
    weight[...] = spread[band:, :]
    spread[...] = jnp.zeros_like(spread)

    def one(k, carry):
        row, col = rows_s[k], cols_s[k]
        win_r, win_i = cut(0, row, col), cut(1, row, col)
        real = probe[0] * win_r - probe[1] * win_i
        imag = probe[0] * win_i + probe[1] * win_r
        real, imag = side(tables, real, imag, False, True)
        real, imag = side(tables, real, imag, False, False)
        factor = 1.0 - measured[k] * lax.rsqrt(real * real + imag * imag + 0.25)
        real, imag = side(tables, real * factor, imag * factor, True, True)
        real, imag = side(tables, real, imag, True, False)
        win_r, win_i = cut(0, row, col), cut(1, row, col)
        grad[0] += win_r * real + win_i * imag
        grad[1] += win_r * imag - win_i * real
        at, x = place(probe[0] * real + probe[1] * imag, row, col)
        totals[0, at, :] += x
        at, x = place(probe[0] * imag - probe[1] * real, row, col)
        totals[1, at, :] += x
        at, x = place(power(), row, col)
        spread[at, :] += x
        return carry

    lax.fori_loop(0, count_s[0], one, 0)
    weight[...] += spread[:band, :]


def on_device(object_field, probe, amplitudes, row_offset, col_offset, frame_count):
    _, band, width = object_field.shape
    frame = probe.shape[1]
    rows, cols, count = row_offset[0, 0], col_offset[0, 0], frame_count[0]
    rim = from_behind(object_field, "dev", -1)
    prior = from_behind(jnp.concatenate([rows, cols, count]), "dev", 1)
    smem = pl.BlockSpec(memory_space=pltpu.SMEM)
    vmem = pl.BlockSpec(memory_space=pltpu.VMEM)
    totals, weight, gradient = pl.pallas_call(
        kernel,
        out_shape=(
            jax.ShapeDtypeStruct((2, band + frame, width), jnp.float32),
            jax.ShapeDtypeStruct((band, width), jnp.float32),
            jax.ShapeDtypeStruct((2, frame, frame), jnp.float32),
        ),
        in_specs=[smem] * 4 + [vmem] * 5,
        out_specs=(vmem,) * 3,
        scratch_shapes=[
            pltpu.VMEM((2, band + frame, width), jnp.float32),
            pltpu.VMEM((band + frame, width), jnp.float32),
        ],
        compiler_params=pltpu.CompilerParams(vmem_limit_bytes=48 * 1024 * 1024),
    )(rows, cols, count, prior, object_field, rim, probe, amplitudes[0, 0], fourier_tables(frame))
    incoming = from_behind(totals[:, band:], "dev", 1)
    new_field = object_field - (totals[:, :band] + incoming) / (weight + 1.0)
    summed = lax.psum(gradient, ("region", "dev"))
    step_scale = 0.25 / jnp.sqrt(jnp.sum(summed * summed) / summed.size + 1e-06)
    return new_field, probe - step_scale * summed


def solution(mesh):
    return jax.shard_map(
        on_device,
        mesh=mesh,
        in_specs=(
            P(None, ("region", "dev"), None),
            P(),
            P("region", "dev", None, None, None),
            P("region", "dev", None),
            P("region", "dev", None),
            P("region", "dev"),
        ),
        out_specs=(P(None, ("region", "dev"), None), P()),
        check_vma=False,
    )
```

```python
import math

import jax
import jax.numpy as jnp
import numpy as np
from jax import lax
from jax.experimental import pallas as pl
from jax.experimental.pallas import tpu as pltpu
from jax.sharding import PartitionSpec as P

PAD = 8


def from_behind(array, axis, by):
    peers = lax.axis_size(axis)
    pairs = [(i, i + by) for i in range(peers) if 0 <= i + by < peers]
    return lax.ppermute(array, axis, pairs)


def summed_over(array, axes):
    if any(lax.axis_size(axis) & (lax.axis_size(axis) - 1) for axis in axes):
        return lax.psum(array, axes)
    steps = []
    for axis in axes:
        size, bit = lax.axis_size(axis), 1
        while bit < size:
            steps.append((axis, bit, [(i, i ^ bit) for i in range(size)]))
            bit *= 2
    shape = array.shape
    share = array.reshape(-1, shape[-1])
    if share.shape[0] % (1 << len(steps)):
        return lax.psum(array, axes)
    for axis, bit, pairs in steps:
        half = share.shape[0] // 2
        upper = (lax.axis_index(axis) & bit) != 0
        low, high = share[:half], share[half:]
        arrived = lax.ppermute(jnp.where(upper, low, high), axis, pairs)
        share = jnp.where(upper, high, low) + arrived
    for axis, bit, pairs in reversed(steps):
        upper = (lax.axis_index(axis) & bit) != 0
        arrived = lax.ppermute(share, axis, pairs)
        share = jnp.concatenate([jnp.where(upper, arrived, share), jnp.where(upper, share, arrived)])
    return share.reshape(shape)


def split(x):
    high = x.astype(jnp.bfloat16)
    return high, (x - high.astype(jnp.float32)).astype(jnp.bfloat16)


def fourier_tables(length):
    index = np.arange(length)
    angle = (index[:, None] * index[None, :] % length) * (2.0 * math.pi / length)
    factor = 1.0 / math.sqrt(length)
    cosine = np.cos(angle) * factor
    sine = np.sin(angle) * factor
    parts = []
    for table in (cosine, sine, cosine + sine, cosine - sine):
        table = table.astype(np.float32)
        high = table.astype(jnp.bfloat16)
        parts += [high, (table - high.astype(np.float32)).astype(jnp.bfloat16)]
    return jnp.asarray(np.stack(parts))


def dot(a, b):
    return jnp.dot(a, b, preferred_element_type=jnp.float32)


def product(tables, which, x, left):
    t_high, t_low = tables[2 * which], tables[2 * which + 1]
    high, low = split(x)
    if left:
        return dot(t_high, high) + (dot(t_high, low) + dot(t_low, high))
    return dot(high, t_high) + (dot(low, t_high) + dot(high, t_low))


def side(tables, real, imag, inverse, left):
    first = product(tables, 2 if inverse else 3, real, left)
    second = product(tables, 0, imag - real, left)
    third = product(tables, 1, real + imag, left)
    if inverse:
        return first - third, first + second
    return first + third, first + second


def kernel(
    rows_s, cols_s, count_s, prior_s, field, rim, probe, measured, tables,
    totals, weight, grad, extended, spread,
):
    band, width = field.shape[1], field.shape[2]
    frame = probe.shape[1]
    slots = rows_s.shape[0]
    tall = frame + PAD
    extended[:, :band] = field[...]
    extended[:, band:] = rim[...]
    totals[...] = jnp.zeros_like(totals)
    spread[...] = jnp.zeros_like(spread)
    grad[...] = jnp.zeros_like(grad)

    def anchor(row):
        base = pl.multiple_of(row // PAD * PAD, PAD)
        return pl.ds(base, tall), row - base

    def cut(plane, row, col):
        at, shift = anchor(row)
        x = extended[plane, at, :]
        x = pltpu.roll(x, lax.rem(width - col, width), 1)[:, :frame]
        return pltpu.roll(x, lax.rem(tall - shift, tall), 0)[:frame]

    def place(x, row, col):
        at, shift = anchor(row)
        x = jnp.concatenate([x, jnp.zeros((PAD, frame), jnp.float32)], axis=0)
        x = pltpu.roll(x, shift, 0)
        x = jnp.concatenate([x, jnp.zeros((tall, width - frame), jnp.float32)], axis=1)
        return at, pltpu.roll(x, col, 1)

    def power():
        return probe[0] * probe[0] + probe[1] * probe[1]

    def prior(k, carry):
        at, x = place(power(), prior_s[k], prior_s[slots + k])
        spread[at, :] += x
        return carry

    lax.fori_loop(0, prior_s[2 * slots], prior, 0)
    weight[...] = spread[band:, :]
    spread[...] = jnp.zeros_like(spread)

    def one(k, carry):
        row, col = rows_s[k], cols_s[k]
        win_r, win_i = cut(0, row, col), cut(1, row, col)
        real = probe[0] * win_r - probe[1] * win_i
        imag = probe[0] * win_i + probe[1] * win_r
        real, imag = side(tables, real, imag, False, True)
        real, imag = side(tables, real, imag, False, False)
        factor = 1.0 - measured[k] * lax.rsqrt(real * real + imag * imag + 0.25)
        real, imag = side(tables, real * factor, imag * factor, True, True)
        real, imag = side(tables, real, imag, True, False)
        win_r, win_i = cut(0, row, col), cut(1, row, col)
        grad[0] += win_r * real + win_i * imag
        grad[1] += win_r * imag - win_i * real
        at, x = place(probe[0] * real + probe[1] * imag, row, col)
        totals[0, at, :] += x
        at, x = place(probe[0] * imag - probe[1] * real, row, col)
        totals[1, at, :] += x
        at, x = place(power(), row, col)
        spread[at, :] += x
        return carry

    lax.fori_loop(0, count_s[0], one, 0)
    weight[...] += spread[:band, :]


def on_device(object_field, probe, amplitudes, row_offset, col_offset, frame_count):
    _, band, width = object_field.shape
    frame = probe.shape[1]
    rows, cols, count = row_offset[0, 0], col_offset[0, 0], frame_count[0]
    rim = from_behind(object_field, "dev", -1)
    prior = from_behind(jnp.concatenate([rows, cols, count]), "dev", 1)
    smem = pl.BlockSpec(memory_space=pltpu.SMEM)
    vmem = pl.BlockSpec(memory_space=pltpu.VMEM)
    totals, weight, gradient = pl.pallas_call(
        kernel,
        out_shape=(
            jax.ShapeDtypeStruct((2, band + frame, width), jnp.float32),
            jax.ShapeDtypeStruct((band, width), jnp.float32),
            jax.ShapeDtypeStruct((2, frame, frame), jnp.float32),
        ),
        in_specs=[smem] * 4 + [vmem] * 5,
        out_specs=(vmem,) * 3,
        scratch_shapes=[
            pltpu.VMEM((2, band + frame, width), jnp.float32),
            pltpu.VMEM((band + frame, width), jnp.float32),
        ],
        compiler_params=pltpu.CompilerParams(vmem_limit_bytes=48 * 1024 * 1024),
    )(rows, cols, count, prior, object_field, rim, probe, amplitudes[0, 0], fourier_tables(frame))
    incoming = from_behind(totals[:, band:], "dev", 1)
    new_field = object_field - (totals[:, :band] + incoming) / (weight + 1.0)
    summed = summed_over(gradient, ("dev", "region"))
    step_scale = 0.25 / jnp.sqrt(jnp.sum(summed * summed) / summed.size + 1e-06)
    return new_field, probe - step_scale * summed


def solution(mesh):
    return jax.shard_map(
        on_device,
        mesh=mesh,
        in_specs=(
            P(None, ("region", "dev"), None),
            P(),
            P("region", "dev", None, None, None),
            P("region", "dev", None),
            P("region", "dev", None),
            P("region", "dev"),
        ),
        out_specs=(P(None, ("region", "dev"), None), P()),
        check_vma=False,
    )
```
